32 devices in a mesh: units: 8 (over z, x), expert: 4 (over y, core).
Axes of the slice: x: 2, y: 2, z: 4, core: 2. Of those that a mesh axis runs over, the one named last changes fastest.
Arguments:
- a_up: float32 [57344, 2048], P(('expert', 'units')), parts along dimension 0, may hold values from -6 to 6
- a_down: float32 [57344, 2048], P(('expert', 'units')), parts along dimension 0, may hold values from -6 to 6
- b_up: float32 [57344, 2048], P(('expert', 'units')), parts along dimension 0, may hold values from -6 to 6
- b_down: float32 [57344, 2048], P(('expert', 'units')), parts along dimension 0, may hold values from -6 to 6
- perm: int32 [57344], P('expert'), parts along dimension 0, may hold values from 0 to 14335, as said below
Outputs:
- merged_up: float32 [57344, 2048], P(('expert', 'units')), parts along dimension 0
- merged_down: float32 [57344, 2048], P(('expert', 'units')), parts along dimension 0
The draws below stay inside these ranges and needn't reach their ends.
There are 4 independent parts, one for each index of `expert`. The reference program is written for one: setup_inputs(seed, part) draws one part's arguments, and reference() takes and returns one part's arrays. A program takes and returns all parts, laid end to end along the dimension named above; each array names one. Nothing has to cross between parts.
Inputs may be any that keep to these rules, and one draw needn't show every extreme that they name: perm names each of the 14336 units once. Cut the units into aligned blocks of 1792: of the units of one source block, at most 225 are matched to units of any one destination block, and in every draw some pair of blocks reaches 225. Every source block sends the same list of counts to the destination blocks, in an order that differs from source to source.
All inputs are finite; a program needn't handle non-finite values.
Results may differ from the reference program's by a relative error of at most 0.00002.
Values sent between devices are 32-bit elements; how exact they have to be, the bound alone decides.
A program may use at most 192 MiB of HBM per device.

```python
import jax
import jax.numpy as jnp

FF = 14336
DW = 2048
CAP = 225
N_UNITS = 8


def draw_perm(key, part):
    per_dev = FF // N_UNITS
    count = N_UNITS
    limit = CAP
    keys = jax.random.split(jax.random.fold_in(key, 7), 6)
    spans = jax.random.randint(keys[0], (count,), limit - 1, limit + 1).astype(jnp.int32)
    spans = spans.at[0].set(limit)
    taken = jnp.cumsum(spans) - spans
    pieces = jnp.clip(per_dev - taken, 0, spans).astype(jnp.int32)
    ends = jnp.cumsum(pieces)
    slot = jnp.arange(per_dev, dtype=jnp.int32)
    which = jnp.sum((slot[:, None] >= ends[None, :]).astype(jnp.int32), axis=1)
    sigma = jax.random.permutation(keys[1], count).astype(jnp.int32)
    tau = jax.random.permutation(keys[2], count).astype(jnp.int32)
    sigma_inv = jnp.argsort(sigma).astype(jnp.int32)
    tau_inv = jnp.argsort(tau).astype(jnp.int32)
    source_order = jax.vmap(lambda subkey: jax.random.permutation(subkey, per_dev))(jax.random.split(keys[3], count)).astype(jnp.int32)
    target_order = jax.vmap(lambda subkey: jax.random.permutation(subkey, per_dev))(jax.random.split(keys[4], count)).astype(jnp.int32)
    dest = jnp.arange(count, dtype=jnp.int32)[:, None]
    source = tau_inv[(sigma_inv[dest] - which[None, :]) % count]
    dest_rows = dest * per_dev + target_order
    source_rows = source * per_dev + source_order[source, slot[None, :]]
    result = jnp.zeros((count * per_dev,), jnp.int32).at[dest_rows.reshape(-1)].set(source_rows.reshape(-1))
    return result


def shard_levels(key, shape, cuts, smallest, high):
    level = 1.0
    for axis_at, shards_of in cuts:
        steps = jax.random.uniform(jax.random.fold_in(jax.random.fold_in(key, 6), axis_at), (shards_of,), jnp.float32, smallest / len(cuts), high / len(cuts))
        level = level * jnp.repeat(jnp.exp(steps), shape[axis_at] // shards_of).reshape((-1,) + (1,) * (len(shape) - 1 - axis_at))
    return level


def bell_draw(stream_key, extent, deviation, reach, cuts=(), kind=jnp.bfloat16):
    array = jax.random.normal(stream_key, extent, jnp.float32) * deviation
    if len(cuts) > 0:
        array = shard_levels(stream_key, extent, cuts, -0.22, 0.18) * array
    return jnp.clip(array, min=-reach, max=reach).astype(kind)


def setup_inputs(seed: int = 0, part: int = 0) -> dict:
    key_of = jax.random.split(jax.random.key(seed), 6)
    own_keys = jax.random.split(jax.random.fold_in(key_of[5], part), 6)
    a_up = bell_draw(own_keys[0], (FF, DW), 1.0, 6.0, ((0, 8),), jnp.float32)
    a_down = bell_draw(own_keys[1], (FF, DW), 1.0, 6.0, ((0, 8),), jnp.float32)
    b_up = bell_draw(own_keys[2], (FF, DW), 1.0, 6.0, ((0, 8),), jnp.float32)
    b_down = bell_draw(own_keys[3], (FF, DW), 1.0, 6.0, ((0, 8),), jnp.float32)
    perm = draw_perm(jax.random.fold_in(jax.random.fold_in(key_of[5], part), 71), part)
    return {"a_up": a_up, "a_down": a_down, "b_up": b_up, "b_down": b_down, "perm": perm}


def reference(a_up, a_down, b_up, b_down, perm):
    permuted_up = jnp.take(b_up, perm, axis=0)
    permuted_down = jnp.take(b_down, perm, axis=0)
    merged_up = (a_up + permuted_up) * 0.5
    merged_down = (a_down + permuted_down) * 0.5
    return merged_up, merged_down
```

```python
import functools

import jax
import jax.numpy as jnp
from jax import lax
from jax.experimental import pallas as pl
from jax.experimental.pallas import tpu as pltpu
from jax.sharding import PartitionSpec as P

LANES = 256
UNROLL = 25


def index_lists(perm, rows, count, limit, me):
    base = me * rows
    table = perm.reshape(count, rows)
    mine = (table >= base) & (table < base + rows)
    upto = jnp.arange(rows, dtype=jnp.int32)
    earlier = (upto[:, None] < upto[None, :]).astype(jnp.bfloat16)
    rank = jnp.dot(mine.astype(jnp.bfloat16), earlier, preferred_element_type=jnp.float32).astype(jnp.int32)
    rank = jnp.where(mine, rank, -1)
    local = jnp.where(mine, table - base, 0)
    ids = jnp.arange(limit, dtype=jnp.int32)
    slots = jnp.sum(jnp.where(rank[:, None, :] == ids[None, :, None], local[:, None, :], 0), axis=2)

    sources = lax.dynamic_slice_in_dim(perm, base, rows)
    owner = sources // rows
    ids_dev = jnp.arange(count, dtype=jnp.int32)
    from_dev = owner[None, :] == ids_dev[:, None]
    place = jnp.dot(from_dev.astype(jnp.bfloat16), earlier, preferred_element_type=jnp.float32).astype(jnp.int32)
    place = jnp.sum(jnp.where(from_dev, place, 0), axis=0)
    return slots.reshape(-1), owner, place


def pack_kernel(count, limit, slots_ref, b_ref, out_ref):
    def one(dest, k):
        row = slots_ref[dest * limit + k]
        out_ref[dest, pl.ds(k, 1), :] = b_ref[pl.ds(row, 1), :]

    step = min(UNROLL, limit)

    @pl.loop(0, count)
    def _(dest):
        @pl.loop(0, limit // step)
        def _(group):
            for u in range(step):
                one(dest, group * step + u)

        for k in range(limit // step * step, limit):
            one(dest, k)


def pack(matrix, slots, count, limit, first, tiles):
    rows, columns = matrix.shape
    return pl.pallas_call(
        functools.partial(pack_kernel, count, limit),
        out_shape=jax.ShapeDtypeStruct((count, limit, tiles * LANES), matrix.dtype),
        grid_spec=pltpu.PrefetchScalarGridSpec(
            num_scalar_prefetch=1,
            grid=(tiles,),
            in_specs=[pl.BlockSpec((rows, LANES), lambda t, s: (0, first + t))],
            out_specs=pl.BlockSpec((count, limit, LANES), lambda t, s: (0, 0, t)),
        ),
        cost_estimate=pl.CostEstimate(flops=0, bytes_accessed=4 * rows * tiles * LANES * 4, transcendentals=0),
        name="pack_rows",
    )(slots, matrix)


def unpack_kernel(rows, owner_ref, place_ref, got_ref, a_ref, *rest):
    out_ref = rest[-1]
    step = 16 if rows % 16 == 0 else 1

    @pl.loop(0, rows // step)
    def _(group):
        for u in range(step):
            j = group * step + u
            value = got_ref[owner_ref[j], pl.ds(place_ref[j], 1), :]
            out_ref[pl.ds(j, 1), :] = (a_ref[pl.ds(j, 1), :] + value) * 0.5


def unpack(got, own, owner, place, first, so_far):
    count, limit, width = got.shape
    rows, columns = own.shape
    tiles = width // LANES
    operands = [owner, place, got, own]
    in_specs = [
        pl.BlockSpec((count, limit, LANES), lambda t, o, p: (0, 0, t)),
        pl.BlockSpec((rows, LANES), lambda t, o, p: (0, first + t)),
    ]
    aliases = {}
    if so_far is not None:
        operands.append(so_far)
        in_specs.append(pl.BlockSpec(memory_space=pl.ANY))
        aliases = {4: 0}
    return pl.pallas_call(
        functools.partial(unpack_kernel, rows),
        out_shape=jax.ShapeDtypeStruct(own.shape, own.dtype),
        grid_spec=pltpu.PrefetchScalarGridSpec(
            num_scalar_prefetch=2,
            grid=(tiles,),
            in_specs=in_specs,
            out_specs=pl.BlockSpec((rows, LANES), lambda t, o, p: (0, first + t)),
        ),
        input_output_aliases=aliases,
        cost_estimate=pl.CostEstimate(flops=0, bytes_accessed=5 * rows * width * 4, transcendentals=0),
        name="merge_rows",
    )(*operands)


def on_device(widths, a_up, a_down, b_up, b_down, perm):
    count = lax.axis_size("units")
    me = lax.axis_index("units")
    rows, columns = b_up.shape
    limit = (rows + count - 1) // count + 1
    slots, owner, place = index_lists(perm, rows, count, limit, me)
    pieces = [("up", first, width) for first, width in widths(columns)]
    pieces += [("down", first, width) for first, width in reversed_order(widths(columns))]
    a = {"up": a_up, "down": a_down}
    b = {"up": b_up, "down": b_down}
    out = {"up": None, "down": None}
    gots = []
    for name, first, tiles in pieces:
        packed = pack(b[name], slots, count, limit, first, tiles)
        gots.append(lax.all_to_all(packed, "units", split_axis=0, concat_axis=0, tiled=True))
    for (name, first, tiles), got in zip(pieces, gots):
        out[name] = unpack(got, a[name], owner, place, first, out[name])
    return out["up"], out["down"]


def widths(columns):
    total = columns // LANES
    first = max(total // 4, 1)
    return ((0, first), (first, total - first))


def reversed_order(parts):
    total = sum(width for _, width in parts)
    return tuple((total - first - width, width) for first, width in reversed(parts))


def solution(mesh):
    split = P(("expert", "units"), None)
    return jax.shard_map(
        functools.partial(on_device, widths),
        mesh=mesh,
        in_specs=(split, split, split, split, P("expert")),
        out_specs=(split, split),
        check_vma=False,
    )
```

```python
import functools

import jax
import jax.numpy as jnp
from jax import lax
from jax.experimental import pallas as pl
from jax.experimental.pallas import tpu as pltpu
from jax.sharding import PartitionSpec as P


LANES = 512
BATCH = 8


def peers(count):
    return [(count - p) % count for p in range(count)]


def index_lists(perm, rows, count, limit, me):
    base = me * rows
    table = perm.reshape(count, rows)
    mine = (table >= base) & (table < base + rows)
    upto = jnp.arange(rows, dtype=jnp.int32)
    earlier = (upto[:, None] < upto[None, :]).astype(jnp.bfloat16)
    rank = jnp.dot(mine.astype(jnp.bfloat16), earlier, preferred_element_type=jnp.float32).astype(jnp.int32)
    rank = jnp.where(mine, rank, -1)
    local = jnp.where(mine, table - base, 0)
    ids = jnp.arange(limit, dtype=jnp.int32)
    slots = jnp.sum(jnp.where(rank[:, None, :] == ids[None, :, None], local[:, None, :], 0), axis=2)

    sources = lax.dynamic_slice_in_dim(perm, base, rows)
    owner = sources // rows
    ids_dev = jnp.arange(count, dtype=jnp.int32)
    from_dev = owner[None, :] == ids_dev[:, None]
    place = jnp.dot(from_dev.astype(jnp.bfloat16), earlier, preferred_element_type=jnp.float32).astype(jnp.int32)
    place = jnp.sum(jnp.where(from_dev, place, 0), axis=0)
    padded = (limit + 7) // 8 * 8
    place_of = (count - (owner ^ me)) % count
    return slots.reshape(-1), place_of * padded + place


def pack_kernel(count, limit, slots_ref, me_ref, b_ref, *out_refs):
    def some(out_ref, base, first, size):
        values = [b_ref[pl.ds(slots_ref[base + first + u], 1), :] for u in range(size)]
        for u in range(size):
            out_ref[pl.ds(first + u, 1), :] = values[u]

    for out_ref, k in zip(out_refs, peers(count)):
        base = (me_ref[0] ^ k) * limit

        @pl.loop(0, limit // BATCH)
        def _(group):
            some(out_ref, base, pl.multiple_of(group * BATCH, BATCH), BATCH)

        if limit % BATCH:
            some(out_ref, base, limit // BATCH * BATCH, limit % BATCH)


def pack(matrix, slots, me, count, limit, first, tiles):
    rows, _ = matrix.shape
    return pl.pallas_call(
        functools.partial(pack_kernel, count, limit),
        out_shape=[jax.ShapeDtypeStruct((limit, tiles * LANES), matrix.dtype)] * count,
        grid_spec=pltpu.PrefetchScalarGridSpec(
            num_scalar_prefetch=2,
            grid=(tiles,),
            in_specs=[pl.BlockSpec((rows, LANES), lambda t, s, m: (0, first + t))],
            out_specs=[pl.BlockSpec((limit, LANES), lambda t, s, m: (0, t))] * count,
        ),
        cost_estimate=pl.CostEstimate(flops=0, bytes_accessed=4 * rows * tiles * LANES * 4, transcendentals=0),
        name="pack_rows",
    )(slots, me.reshape(1), matrix)


def merge_kernel(count, limit, picks_ref, *refs):
    got_refs, a_ref, out_ref, table = refs[:count], refs[count], refs[-2], refs[-1]
    rows = a_ref.shape[0]
    padded = table.shape[0] // count
    for k in range(count):
        table[pl.ds(k * padded, limit), :] = got_refs[k][...]

    @pl.loop(0, rows // BATCH)
    def _(group):
        first = pl.multiple_of(group * BATCH, BATCH)
        values = [table[pl.ds(picks_ref[first + u], 1), :] for u in range(BATCH)]
        owns = [a_ref[pl.ds(first + u, 1), :] for u in range(BATCH)]
        for u in range(BATCH):
            out_ref[pl.ds(first + u, 1), :] = (owns[u] + values[u]) * 0.5


def merge(gots, own, picks, first, so_far):
    count = len(gots)
    limit, width = gots[0].shape
    rows, _ = own.shape
    tiles = width // LANES
    padded = (limit + 7) // 8 * 8
    operands = [picks, *gots, own]
    in_specs = [pl.BlockSpec((limit, LANES), lambda t, p: (0, t))] * count
    in_specs.append(pl.BlockSpec((rows, LANES), lambda t, p: (0, first + t)))
    aliases = {}
    if so_far is not None:
        aliases = {len(operands): 0}
        operands.append(so_far)
        in_specs.append(pl.BlockSpec(memory_space=pl.ANY))
    return pl.pallas_call(
        functools.partial(merge_kernel, count, limit),
        out_shape=jax.ShapeDtypeStruct(own.shape, own.dtype),
        grid_spec=pltpu.PrefetchScalarGridSpec(
            num_scalar_prefetch=1,
            grid=(tiles,),
            in_specs=in_specs,
            out_specs=pl.BlockSpec((rows, LANES), lambda t, p: (0, first + t)),
            scratch_shapes=[pltpu.VMEM((count * padded, LANES), own.dtype)],
        ),
        input_output_aliases=aliases,
        cost_estimate=pl.CostEstimate(flops=0, bytes_accessed=6 * rows * width * 4, transcendentals=0),
        name="merge_rows",
    )(*operands)


def exchange(parts, count, me):
    order = peers(count)
    if count <= 8:
        got = [lax.ppermute(part, "units", [(i, i ^ k) for i in range(count)]) for part, k in zip(parts[1:], order[1:])]
        return [parts[0], *got]
    places = (count - (jnp.arange(count, dtype=jnp.int32) ^ me)) % count
    back = lax.all_to_all(jnp.take(jnp.stack(parts), places, axis=0), "units", split_axis=0, concat_axis=0, tiled=True)
    back = jnp.take(back, jnp.array(order, jnp.int32) ^ me, axis=0)
    return [back[k] for k in range(count)]


def pieces_of(columns):
    total = columns // LANES
    sizes = [1, 1, total - 2] if total > 2 else [total]
    plan = []
    for which, widths in ((0, sizes), (1, sizes[::-1])):
        first = 0
        for tiles in widths:
            plan.append((which, first, tiles))
            first += tiles
    return plan


def on_device(a_up, a_down, b_up, b_down, perm):
    count = lax.axis_size("units")
    me = lax.axis_index("units")
    rows, columns = b_up.shape
    limit = (rows + count - 1) // count + 1
    slots, picks = index_lists(perm, rows, count, limit, me)
    own, other, out = (a_up, a_down), (b_up, b_down), [None, None]
    gots = []
    plan = pieces_of(columns)
    for at, (which, first, tiles) in enumerate(plan):
        parts = pack(other[which], slots, me, count, limit, first, tiles)
        slots, parts = lax.optimization_barrier((slots, parts))
        if at >= 3:
            parts, gots[at - 3] = lax.optimization_barrier((parts, gots[at - 3]))
        gots.append(exchange(parts, count, me))
    for at, (which, first, tiles) in enumerate(plan):
        merged = merge(gots[at], own[which], picks, first, out[which])
        picks, out[which] = lax.optimization_barrier((picks, merged))
    return out[0], out[1]


def solution(mesh):
    split = P(("expert", "units"), None)
    return jax.shard_map(
        on_device,
        mesh=mesh,
        in_specs=(split, split, split, split, P("expert")),
        out_specs=(split, split),
        check_vma=False,
    )
```
